32 devices in a mesh: section: 4 (over x, core), ep: 8 (over z, y).
Axes of the slice: x: 2, y: 2, z: 4, core: 2. Of those that a mesh axis runs over, the one named last changes fastest.
Arguments:
- hidden_states: bfloat16 [384, 6144], P('ep'), may hold values from -6 to 6
- route_experts: int32 [384, 2], P('ep'), may hold values from 0 to 7, all different within a row; in each aligned block of 48 rows (0 to 47, 48 to 95, ...) at most 24 rows name the same one
- route_weights: float32 [384, 2], P('ep'), may hold values from 0.05 to 1
- gate_weight: bfloat16 [8, 6144, 8192], P('ep', None, 'section'), may hold values from -0.078125 to 0.078125
- up_weight: bfloat16 [8, 6144, 8192], P('ep', None, 'section'), may hold values from -0.078125 to 0.078125
- down_weight: bfloat16 [8, 8192, 6144], P('ep', 'section'), may hold values from -0.0625 to 0.0625
Outputs:
- layer_out: bfloat16 [384, 6144], P('ep', 'section')
The draws below stay inside these ranges and needn't reach their ends.
Inputs may be any that keep to these rules, and one draw needn't show every extreme that they name: `route_experts`: each row names two different experts. Among the 48 rows of one ep index no expert is named by more than 24 rows, and in every draw some expert is named by exactly 24 rows of some ep index.
All inputs are finite; a program needn't handle non-finite values.
Results may differ from the reference program's by a relative error of at most 0.015.
Values may be sent and summed in bfloat16 or wider, within the bound.
A program may use at most 128 MiB of HBM per device.

```python
import math
import jax
import jax.numpy as jnp
import numpy as np
from jax import lax

D = 6144
FF = 8192
EXPERTS = 8
TOK_DEV = 48
TOKENS = 384
CAP = 24
MEMBERS = 1
N_SECTION = 4
N_EP = 8


def levels(key, extent, pieces, smallest, top_value):
    factor_of, own = 1.0, jax.random.fold_in(key, 6)
    for axis_at, blocks in pieces:
        steps = jnp.exp(jax.random.uniform(jax.random.fold_in(own, axis_at), (blocks,), jnp.float32, smallest / len(pieces), top_value / len(pieces)))
        factor_of = factor_of * jnp.repeat(steps, extent[axis_at] // blocks).reshape([-1 if axis == axis_at else 1 for axis in range(len(extent))])
    return factor_of


def routed_block(own_key, own, number, rows, count, top, most, lean):
    ranking = jax.random.permutation(own_key, count)
    packed, ordinary = portions_of(count, rows * top, most, lean, True), portions_of(count, rows * top, most, lean, False)
    places = jnp.arange(count)

    def named(sizes, turn):
        used = int((sizes > 0).sum())
        fixed = max(1, used // 4)
        passed = fixed + (places - fixed + turn * (used - fixed)) % max(1, count - fixed)
        return jnp.zeros((count,), jnp.int32).at[ranking[jnp.where(places < fixed, places, passed)]].set(jnp.asarray(sizes, jnp.int32))

    sizes = jnp.where(number % 4 == 0, named(packed, number // 4), named(ordinary, number - number // 4 - 1))
    mixed = jax.random.permutation(jax.random.fold_in(own, 3), count)
    donor, receiver = mixed[0:count // 2 * 2:2], mixed[1:count // 2 * 2:2]
    margin = jnp.minimum(sizes[donor] - 1, most - sizes[receiver]) // 2
    margin = jnp.where((donor == ranking[0]) | (receiver == ranking[0]) | (sizes[receiver] == 0), 0, jnp.maximum(margin, 0))
    passed = jax.random.randint(jax.random.fold_in(own, 4), (count // 2,), 0, 1 << 20) % (margin + 1)
    sizes = sizes.at[donor].add(-passed).at[receiver].add(passed)
    items = jnp.searchsorted(jnp.cumsum(sizes), jnp.arange(rows * top), side="right").astype(jnp.int32)
    table = items.reshape(top, rows).T
    table = table[jax.random.permutation(jax.random.fold_in(own, 1), rows)]
    turn = jax.random.randint(jax.random.fold_in(own, 2), (rows, 1), 0, top)
    return jnp.take_along_axis(table, (jnp.arange(top)[None, :] + turn) % top, axis=1)


def portions_of(amount, total, limit, lean, full):
    portions = [(1 << 20) // math.isqrt(rank ** lean) + 1 for rank in range(1, amount + 1)]
    largest = limit if full else min(limit, max(-(-total // amount), total * portions[0] // sum(portions)))
    least = 1 if total - largest >= amount - 1 else 0
    holding, spare = [largest] + [least] * (amount - 1), total - largest - least * (amount - 1)
    while spare > 0:
        candidates = [i for i in range(1, amount) if holding[i] < largest] or [i for i in range(1, amount) if holding[i] < limit]
        pool, budget = sum([portions[i] for i in candidates]), spare
        for i in candidates:
            extra = min(limit - holding[i], max(1, budget * portions[i] // pool), spare)
            holding[i] = holding[i] + extra
            spare = spare - extra
    return np.array(holding)


def gaussian(own_key, shape, spread, limit, cuts=(), held_as=jnp.bfloat16):
    drawn = spread * jax.random.normal(own_key, shape, jnp.float32)
    if cuts:
        drawn = drawn * levels(own_key, shape, cuts, -0.22, 0.18)
    return jnp.clip(drawn, -limit, limit).astype(held_as)


def setup_inputs(seed: int = 0) -> dict:
    streams_of = jax.random.split(jax.random.key(seed), 7)
    hidden_states = gaussian(streams_of[0], (TOKENS, D), 1.0, 6.0, ((0, 8),))
    route_experts_keys = jax.random.split(jax.random.fold_in(streams_of[1], 1), TOKENS // TOK_DEV)
    route_experts_turns = jax.random.permutation(jax.random.fold_in(streams_of[1], 3), TOKENS // TOK_DEV)
    route_experts = jax.vmap(lambda own, number: routed_block(jax.random.fold_in(streams_of[1], 2), own, number, TOK_DEV, EXPERTS, 2, CAP, 2))(route_experts_keys, route_experts_turns).reshape((TOKENS, 2))
    route_weights = jnp.clip(0.05 + 0.95 * jax.random.uniform(streams_of[2], (TOKENS, 2), jnp.float32) ** levels(streams_of[2], (TOKENS, 2), ((0, 8),), -0.2, 0.2), 0.05, 1.0)
    gate_weight = gaussian(streams_of[3], (N_EP, D, FF // MEMBERS), D ** -0.5, 0.078125, ((0, 8), (2, 4)))
    up_weight = gaussian(streams_of[4], (N_EP, D, FF // MEMBERS), D ** -0.5, 0.078125, ((0, 8), (2, 4)))
    down_weight = gaussian(streams_of[5], (N_EP, FF // MEMBERS, D), FF ** -0.5, 0.0625, ((0, 8), (1, 4)))
    return dict(hidden_states=hidden_states, route_experts=route_experts, route_weights=route_weights, gate_weight=gate_weight, up_weight=up_weight, down_weight=down_weight)


def shard_output(slot_rows, gate_block, up_block, down_block):
    gate_value = jnp.dot(slot_rows, gate_block, preferred_element_type=jnp.float32)
    up_value = jnp.dot(slot_rows, up_block, preferred_element_type=jnp.float32)
    hidden = (jax.nn.silu(gate_value) * up_value).astype(jnp.bfloat16)
    return jnp.dot(hidden, down_block, preferred_element_type=jnp.float32).astype(jnp.bfloat16).astype(jnp.float32)


def reference(hidden_states, route_experts, route_weights, gate_weight, up_weight, down_weight):
    members = N_EP // EXPERTS
    capacity = TOK_DEV // 2
    shard_width = gate_weight.shape[2] // N_SECTION
    blocks = route_experts.reshape(N_EP, TOK_DEV * 2)
    labels = jnp.arange(EXPERTS, dtype=jnp.int32)
    one_hot = (blocks[:, :, None] == labels[None, None, :]).astype(jnp.int32)
    earlier = jnp.cumsum(one_hot, axis=1) - one_hot
    slot_index = jnp.sum(earlier * one_hot, axis=2)
    entry = jnp.arange(TOK_DEV * 2, dtype=jnp.int32)
    token_row = jnp.arange(N_EP, dtype=jnp.int32)[:, None] * TOK_DEV + entry[None, :] // 2
    flat_weights = route_weights.reshape(N_EP, TOK_DEV * 2)
    slots = jnp.arange(capacity, dtype=jnp.int32)
    result = jnp.zeros((TOKENS, D), jnp.float32)
    for expert in range(EXPERTS):
        matches = ((blocks[:, None, :] == expert) & (slot_index[:, None, :] == slots[None, :, None])).astype(jnp.int32)
        rows_index = jnp.sum(matches * token_row[:, None, :], axis=2).reshape(-1).astype(jnp.int32)
        weight_slot = jnp.sum(matches.astype(jnp.float32) * flat_weights[:, None, :], axis=2).reshape(-1)
        gathered = hidden_states[rows_index]

        def add_shard(shard, total):
            member = shard // N_SECTION
            section_index = shard % N_SECTION
            block_index = (expert * members + member).astype(jnp.int32)
            offset = (section_index * shard_width).astype(jnp.int32)
            gate_block = lax.dynamic_slice_in_dim(lax.dynamic_index_in_dim(gate_weight, block_index, 0, keepdims=False), offset, shard_width, 1)
            up_block = lax.dynamic_slice_in_dim(lax.dynamic_index_in_dim(up_weight, block_index, 0, keepdims=False), offset, shard_width, 1)
            down_block = lax.dynamic_slice_in_dim(lax.dynamic_index_in_dim(down_weight, block_index, 0, keepdims=False), offset, shard_width, 0)
            return total + shard_output(gathered, gate_block, up_block, down_block)

        total = lax.fori_loop(0, members * N_SECTION, add_shard, jnp.zeros((N_EP * capacity, D), jnp.float32))
        result = result.at[rows_index].add(weight_slot[:, None] * total)
    return result.astype(jnp.bfloat16)
```

```python
import functools

import jax
import jax.numpy as jnp
from jax import lax
from jax.experimental import pallas as pl
from jax.experimental.pallas import tpu as pltpu
from jax.sharding import PartitionSpec as P

EXPERTS = 8
CORES = 2
MESH = pl.DeviceIdType.MESH


def fit(size, options):
    return next(o for o in options if size % o == 0)


def kernel(
    E, S, C, D, FFS, tf, ft, NG, ND,
    packed, weigh, gate, up, down, out,
    x_all, gbuf, ubuf, dbuf, hid, psend, prec, pmine, xsend, xrec, own, sumb, ret,
    s1, r1, s2, r2, s3, r3, s4, r4, s5, r5, s6, r6, gs, us, ds, lsem,
):
    nx = S // CORES
    M = E // EXPERTS
    DS = D // S
    NT = DS // ft
    NTF = FFS // tf
    R = E * C
    sec = lax.axis_index("section")
    me = lax.axis_index("ep")
    x, c = sec // CORES, lax.rem(sec, CORES)
    mate = x * CORES + 1 - c
    f32 = jnp.float32

    def gcopy(t):
        slot = lax.rem(t, NG)
        cols = pl.ds(pl.multiple_of(t * tf, tf), tf)
        return (
            pltpu.make_async_copy(gate.at[0, :, cols], gbuf.at[slot], gs.at[slot]),
            pltpu.make_async_copy(up.at[0, :, cols], ubuf.at[slot], us.at[slot]),
        )

    def dcopy(q):
        slot = lax.rem(q, ND)
        xi, f, ci = q // (NT * CORES), lax.rem(q // CORES, NT), lax.rem(q, CORES)
        xd = lax.rem(x + 1 + xi, nx)
        cd = (1 - c) * (1 - ci) + c * ci
        start = (xd * CORES + cd) * DS + f * ft
        cols = pl.ds(pl.multiple_of(start, 128), ft)
        return pltpu.make_async_copy(down.at[0, :, cols], dbuf.at[slot], ds.at[slot])

    for t in range(min(NG, NTF)):
        for cp in gcopy(t):
            cp.start()
    local = pltpu.make_async_copy(packed.at[me // M], x_all.at[sec, me], lsem)
    local.start()

    barrier = pltpu.get_barrier_semaphore()

    def greet(k, _):
        pl.semaphore_signal(barrier, inc=1, device_id=(sec, lax.rem(me + k, E)), device_id_type=MESH)
        return 0

    lax.fori_loop(1, E, greet, 0)
    for j in range(1, nx):
        pl.semaphore_signal(
            barrier, inc=1, device_id=(lax.rem(x + j, nx) * CORES + c, me), device_id_type=MESH
        )
    pl.semaphore_signal(barrier, inc=1, device_id=(mate, me), device_id_type=MESH)
    pl.semaphore_wait(barrier, E - 1 + nx)

    def rcopy(src, dst, ss, rs, dev):
        return pltpu.make_async_remote_copy(
            src_ref=src, dst_ref=dst, send_sem=ss, recv_sem=rs, device_id=dev, device_id_type=MESH
        )

    def c1(k):
        dst = lax.rem(me + k, E)
        return rcopy(packed.at[dst // M], x_all.at[sec, me], s1.at[k], r1.at[k], (sec, dst))

    def c2(j, k):
        src = lax.rem(me - k + E, E)
        piece = x_all.at[sec, src]
        return rcopy(
            piece, piece, s2.at[j, k], r2.at[j, k], (lax.rem(x + j, nx) * CORES + c, me)
        )

    def c3(j, k):
        src = lax.rem(me - k + E, E)
        piece = x_all.at[lax.rem(x - j + nx, nx) * CORES + c, src]
        return rcopy(piece, piece, s3.at[j, k], r3.at[j, k], (mate, me))

    def loop(lo, hi, body):
        def step(i, carry):
            body(i)
            return carry

        lax.fori_loop(lo, hi, step, 0)

    loop(1, E, lambda k: c1(k).start())
    for q in range(min(ND, nx * NT * CORES)):
        dcopy(q).start()

    def spread(k):
        for j in range(1, nx):
            c2(j, k).start()
        c3(0, k).start()

    def relay(k):
        for j in range(1, nx):
            c2(j, k).wait_recv()
            c3(j, k).start()

    local.wait()
    spread(0)

    def forward(k):
        c1(k).wait_recv()
        spread(k)
        relay(k - 1)

    loop(1, E, forward)
    relay(E - 1)

    def settle(k):
        for j in range(nx):
            c3(j, k).wait()
        for j in range(1, nx):
            c2(j, k).wait_send()

    loop(0, E, settle)
    loop(1, E, lambda k: c1(k).wait_send())

    def hidden_tile(t):
        slot = lax.rem(t, NG)
        for cp in gcopy(t):
            cp.wait()
        g = jnp.zeros((R, tf), f32)
        u = jnp.zeros((R, tf), f32)
        for s in range(S):
            rows = x_all[s].reshape(R, DS)
            g += jnp.dot(rows, gbuf[slot, s * DS:(s + 1) * DS], preferred_element_type=f32)
            u += jnp.dot(rows, ubuf[slot, s * DS:(s + 1) * DS], preferred_element_type=f32)
        h = (g / (1.0 + jnp.exp(-g)) * u).astype(jnp.bfloat16)
        hid[:, pl.ds(pl.multiple_of(t * tf, tf), tf)] = h

        @pl.when(t + NG < NTF)
        def _():
            for cp in gcopy(t + NG):
                cp.start()

    loop(0, NTF, hidden_tile)

    def part(q):
        slot = lax.rem(q, ND)
        dcopy(q).wait()
        p = jnp.dot(hid[...], dbuf[slot], preferred_element_type=f32).astype(jnp.bfloat16)

        @pl.when(q + ND < nx * NT * CORES)
        def _():
            dcopy(q + ND).start()

        return p

    def c4(g):
        return rcopy(psend.at[g], prec.at[g], s4.at[g], r4.at[g], (mate, me))

    def c6(i, xi):
        dst = lax.rem(x + 1 + xi, nx) * CORES + c
        return rcopy(xsend.at[i], xrec.at[i], s6.at[i], r6.at[i], (dst, me))

    for xi in range(nx):
        base = xi * NT

        def pair(f, xi=xi, base=base):
            c4(base + f).wait_recv()
            total = pmine[base + f].astype(f32) + prec[base + f].astype(f32)
            if xi < nx - 1:
                xsend[base + f] = total.astype(jnp.bfloat16)
                c6(base + f, xi).start()
            else:
                own[f] = total

        def tile(f, base=base, pair=pair):
            g = base + f
            psend[g] = part(CORES * g)
            c4(g).start()
            pmine[g] = part(CORES * g + 1)

            @pl.when(f > 0)
            def _():
                pair(f - 1)

        loop(0, NT, tile)
        pair(NT - 1)

    def c5(f, k):
        dst = lax.rem(me + k, E)
        return rcopy(sumb.at[f, dst], ret.at[f, me], s5.at[f, k], r5.at[f, k], (sec, dst))

    def finish(f):
        total = own[f]
        for xi in range(nx - 1):
            c6(xi * NT + f, xi).wait_recv()
            total = total + xrec[xi * NT + f].astype(f32)
        sumb[f] = total.astype(jnp.bfloat16).reshape(E, C, ft)
        loop(1, E, lambda k: c5(f, k).start())
        ret[f, me] = sumb[f, me]

    loop(0, NT, finish)

    for f in range(NT):
        loop(1, E, lambda k: c5(f, k).wait())
        out[:, f * ft:(f + 1) * ft] = jnp.dot(
            weigh[...],
            ret[f].reshape(R, ft).astype(f32),
            precision=lax.Precision.HIGHEST,
            preferred_element_type=f32,
        ).astype(jnp.bfloat16)
    loop(0, nx * NT, lambda g: c4(g).wait_send())
    for xi in range(nx - 1):
        loop(0, NT, lambda f: c6(xi * NT + f, xi).wait_send())


def on_device(hidden_states, route_experts, route_weights, gate_weight, up_weight, down_weight):
    E = lax.axis_size("ep")
    S = lax.axis_size("section")
    tok_rows, D = hidden_states.shape
    FFS = gate_weight.shape[2]
    M = E // EXPERTS
    C = tok_rows // 2
    DS = D // S
    chosen = route_experts.reshape(-1)
    one_hot = (chosen[:, None] == jnp.arange(EXPERTS, dtype=jnp.int32)[None, :]).astype(jnp.int32)
    earlier = jnp.cumsum(one_hot, axis=0) - one_hot
    slot_index = jnp.sum(earlier * one_hot, axis=1)
    position = (chosen * C + slot_index).reshape(tok_rows, 2)
    columns = jnp.arange(EXPERTS * C, dtype=jnp.int32)
    matches = position[:, :, None] == columns[None, None, :]
    select = jnp.sum(matches.astype(jnp.int32), axis=1).astype(jnp.bfloat16)
    weighing = jnp.sum(matches.astype(jnp.float32) * route_weights[:, :, None], axis=1)
    mine = lax.dynamic_slice_in_dim(hidden_states, lax.axis_index("section") * DS, DS, 1)
    packed = jnp.einsum("tj,td->jd", select, mine, preferred_element_type=jnp.float32)
    packed = packed.astype(jnp.bfloat16).reshape(EXPERTS, C, DS)
    weigh = jnp.repeat(weighing.reshape(tok_rows, EXPERTS, C), M, axis=1).reshape(tok_rows, E * C)

    R = E * C
    nx = S // CORES
    ft = fit(DS, (512, 384, 256, 128))
    NT = DS // ft
    budget = 58_000_000 - (R * DS * 2 * (S + 3 * nx + 2 * nx + 4) + R * FFS * 2)
    tf = 256 if FFS % 256 == 0 and budget > 25_000_000 else 128
    NTF, NQ = FFS // tf, nx * NT * CORES
    gate_bytes, down_bytes = D * tf * 4, FFS * ft * 2
    ND = max(2, min(NQ, 6, budget // 4 // down_bytes))
    NG = max(2, min(NTF, (budget - ND * down_bytes) // gate_bytes))
    bf16, f32 = jnp.bfloat16, jnp.float32
    dma = pltpu.SemaphoreType.DMA
    nxs = max(1, nx - 1) * NT
    vmem = pl.BlockSpec(memory_space=pltpu.VMEM)
    hbm = pl.BlockSpec(memory_space=pl.ANY)
    return pl.pallas_call(
        functools.partial(kernel, E, S, C, D, FFS, tf, ft, NG, ND),
        out_shape=jax.ShapeDtypeStruct((tok_rows, DS), bf16),
        in_specs=[vmem, vmem, hbm, hbm, hbm],
        out_specs=vmem,
        scratch_shapes=[
            pltpu.VMEM((S, E, C, DS), bf16),
            pltpu.VMEM((NG, D, tf), bf16),
            pltpu.VMEM((NG, D, tf), bf16),
            pltpu.VMEM((ND, FFS, ft), bf16),
            pltpu.VMEM((R, FFS), bf16),
            pltpu.VMEM((nx * NT, R, ft), bf16),
            pltpu.VMEM((nx * NT, R, ft), bf16),
            pltpu.VMEM((nx * NT, R, ft), bf16),
            pltpu.VMEM((nxs, R, ft), bf16),
            pltpu.VMEM((nxs, R, ft), bf16),
            pltpu.VMEM((NT, R, ft), f32),
            pltpu.VMEM((NT, E, C, ft), bf16),
            pltpu.VMEM((NT, E, C, ft), bf16),
            dma((E,)), dma((E,)),
            dma((nx, E)), dma((nx, E)),
            dma((nx, E)), dma((nx, E)),
            dma((nx * NT,)), dma((nx * NT,)),
            dma((NT, E)), dma((NT, E)),
            dma((nxs,)), dma((nxs,)),
            dma((NG,)), dma((NG,)), dma((ND,)),
            dma(()),
        ],
        compiler_params=pltpu.CompilerParams(
            collective_id=0, has_side_effects=True, vmem_limit_bytes=67_043_328
        ),
    )(packed, weigh, gate_weight, up_weight, down_weight)


def solution(mesh):
    return jax.shard_map(
        on_device,
        mesh=mesh,
        in_specs=(
            P("ep", None),
            P("ep", None),
            P("ep", None),
            P("ep", None, "section"),
            P("ep", None, "section"),
            P("ep", "section", None),
        ),
        out_specs=P("ep", "section"),
        check_vma=False,
    )
```
